32 devices in a mesh: dp: 1 (over z), cy: 4 (over y), cx: 8 (over x, core).
Axes of the slice: x: 4, y: 4, z: 1, core: 2. Of those that a mesh axis runs over, the one named last changes fastest.
The devices are a block of a 4x4x8 slice.
Arguments:
- query_rows: bfloat16 [8192, 32, 128], P(('dp', 'cy', 'cx'))
- key_rows: bfloat16 [8192, 8, 128], P(('dp', 'cy', 'cx'))
- value_rows: bfloat16 [8192, 8, 128], P(('dp', 'cy', 'cx'))
- out_rows: bfloat16 [8192, 32, 128], P(('dp', 'cy', 'cx'))
- grad_out: bfloat16 [8192, 32, 128], P(('dp', 'cy', 'cx'))
- log_sum_exp: float32 [8192, 32], P(('dp', 'cy', 'cx'))
Outputs:
- output 1: bfloat16 [8192, 32, 128], P(('dp', 'cy', 'cx'))
- output 2: bfloat16 [8192, 8, 128], P(('dp', 'cy', 'cx'))
- output 3: bfloat16 [8192, 8, 128], P(('dp', 'cy', 'cx'))
All inputs are finite; a program needn't handle non-finite values.
Results may differ from the reference program's by a relative error of at most 0.00402.
Values are sent between devices in bfloat16 or wider.
A program may use at most 768 MiB of HBM per device.

```python
import math
import jax
import jax.numpy as jnp
from jax import lax

Q_HEADS = 32
KV_HEADS = 8
HEAD_DIM = 128
TOK_DEV = 256
CTX_DEVS = 32
ROW_BLOCK = 64
SEQ_LEN = CTX_DEVS * TOK_DEV
CHUNK_LEN = TOK_DEV // 2
GROUP_SIZE = Q_HEADS // KV_HEADS
N_BLOCKS = SEQ_LEN // ROW_BLOCK
SCALING = 1.0 / math.sqrt(HEAD_DIM)


def seq_positions():
    local_idx = jnp.arange(TOK_DEV, dtype=jnp.int32)
    dev_idx = jnp.arange(CTX_DEVS, dtype=jnp.int32)
    piece_id = jnp.where(local_idx[None, :] < CHUNK_LEN, dev_idx[:, None], 2 * CTX_DEVS - 1 - dev_idx[:, None])
    return (piece_id * CHUNK_LEN + local_idx[None, :] % CHUNK_LEN).reshape(SEQ_LEN)


def to_seq_order(row_data):
    split_rows = row_data.reshape((CTX_DEVS, 2, CHUNK_LEN) + row_data.shape[1:])
    return jnp.concatenate([split_rows[:, 0], split_rows[::-1, 1]], axis=0).reshape(row_data.shape)


def to_device_order(row_data):
    split_rows = row_data.reshape((2, CTX_DEVS, CHUNK_LEN) + row_data.shape[1:])
    return jnp.stack([split_rows[0], split_rows[1, ::-1]], axis=1).reshape(row_data.shape)


def forward_stats(q_seq, k_seq, v_seq):
    keys_f32 = k_seq.astype(jnp.float32)
    vals_f32 = v_seq.astype(jnp.float32)
    key_pos = jnp.arange(SEQ_LEN)
    q_blocks = q_seq.reshape(N_BLOCKS, ROW_BLOCK, KV_HEADS, GROUP_SIZE, HEAD_DIM)

    def one_block(block_in):
        q_blk, blk_idx = block_in
        query_pos = blk_idx * ROW_BLOCK + jnp.arange(ROW_BLOCK)
        keep_mask = (query_pos[:, None] >= key_pos[None, :])[None, None]
        scores = jnp.einsum('bkgd,skd->kgbs', q_blk.astype(jnp.float32), keys_f32) * SCALING
        masked = jnp.where(keep_mask, scores, -1e30)
        row_max = jnp.max(masked, axis=-1)
        exp_vals = jnp.exp(masked - row_max[..., None])
        row_sum = jnp.sum(exp_vals, axis=-1)
        prob_b16 = (exp_vals / row_sum[..., None]).astype(jnp.bfloat16)
        out_blk = jnp.einsum('kgbs,skd->bkgd', prob_b16.astype(jnp.float32), vals_f32)
        lse_blk = (row_max + jnp.log(row_sum)).transpose(2, 0, 1)
        return out_blk.astype(jnp.bfloat16).reshape(ROW_BLOCK, Q_HEADS, HEAD_DIM), lse_blk.reshape(ROW_BLOCK, Q_HEADS)

    out_blocks, lse_blocks = lax.map(one_block, (q_blocks, jnp.arange(N_BLOCKS)))
    return out_blocks.reshape(SEQ_LEN, Q_HEADS, HEAD_DIM), lse_blocks.reshape(SEQ_LEN, Q_HEADS)


def setup_inputs(seed: int = 0, part: int = 0) -> dict:
    root_key = jax.random.fold_in(jax.random.key(seed), part)
    sub_keys = jax.random.split(root_key, 6)
    shape_q = (SEQ_LEN, Q_HEADS, HEAD_DIM)
    shape_kv = (SEQ_LEN, KV_HEADS, HEAD_DIM)
    query_f32 = jax.random.normal(sub_keys[0], shape_q, jnp.float32)
    key_mean = jax.random.normal(sub_keys[1], (KV_HEADS, HEAD_DIM), jnp.float32)
    key_f32 = jax.random.normal(sub_keys[2], shape_kv, jnp.float32) + key_mean
    value_mean = jax.random.normal(sub_keys[3], (KV_HEADS, HEAD_DIM), jnp.float32)
    value_f32 = jax.random.normal(sub_keys[4], shape_kv, jnp.float32) + value_mean
    row_pos = seq_positions().astype(jnp.float32)
    dout_f32 = jax.random.normal(sub_keys[5], shape_q, jnp.float32) * jnp.sqrt((row_pos + 1.0) / 4.0)[:, None, None]
    query_rows = query_f32.astype(jnp.bfloat16)
    key_rows = key_f32.astype(jnp.bfloat16)
    value_rows = value_f32.astype(jnp.bfloat16)
    out_seq, lse_seq = forward_stats(to_seq_order(query_rows), to_seq_order(key_rows), to_seq_order(value_rows))
    return {'query_rows': query_rows, 'key_rows': key_rows, 'value_rows': value_rows, 'out_rows': to_device_order(out_seq), 'grad_out': dout_f32.astype(jnp.bfloat16), 'log_sum_exp': to_device_order(lse_seq)}


def reference(query_rows, key_rows, value_rows, out_rows, grad_out, log_sum_exp):
    q_seq = to_seq_order(query_rows)
    keys_f32 = to_seq_order(key_rows).astype(jnp.float32)
    vals_f32 = to_seq_order(value_rows).astype(jnp.float32)
    do_seq = to_seq_order(grad_out)
    delta_seq = jnp.einsum('shd,shd->sh', do_seq.astype(jnp.float32), to_seq_order(out_rows).astype(jnp.float32))
    lse_seq = to_seq_order(log_sum_exp)
    blk_shape = (N_BLOCKS, ROW_BLOCK, KV_HEADS, GROUP_SIZE)
    key_pos = jnp.arange(SEQ_LEN)

    def one_block(grad_acc, block_in):
        dk_acc, dv_acc = grad_acc
        q_blk, do_blk, lse_blk, delta_blk, blk_idx = block_in
        q_f32 = q_blk.astype(jnp.float32)
        do_f32 = do_blk.astype(jnp.float32)
        query_pos = blk_idx * ROW_BLOCK + jnp.arange(ROW_BLOCK)
        keep_mask = (query_pos[:, None] >= key_pos[None, :])[None, None]
        scores = jnp.einsum('bkgd,skd->kgbs', q_f32, keys_f32) * SCALING
        prob_f32 = jnp.where(keep_mask, jnp.exp(scores - lse_blk.transpose(1, 2, 0)[..., None]), 0.0)
        dprob_f32 = jnp.einsum('bkgd,skd->kgbs', do_f32, vals_f32)
        dscore = (prob_f32 * (dprob_f32 - delta_blk.transpose(1, 2, 0)[..., None])).astype(jnp.bfloat16).astype(jnp.float32)
        prob_rnd = prob_f32.astype(jnp.bfloat16).astype(jnp.float32)
        dq_blk = jnp.einsum('kgbs,skd->bkgd', dscore, keys_f32) * SCALING
        dk_acc = dk_acc + jnp.einsum('kgbs,bkgd->skd', dscore, q_f32)
        dv_acc = dv_acc + jnp.einsum('kgbs,bkgd->skd', prob_rnd, do_f32)
        return (dk_acc, dv_acc), dq_blk.astype(jnp.bfloat16).reshape(ROW_BLOCK, Q_HEADS, HEAD_DIM)

    zero_kv = jnp.zeros((SEQ_LEN, KV_HEADS, HEAD_DIM), jnp.float32)
    block_ins = (q_seq.reshape(blk_shape + (HEAD_DIM,)), do_seq.reshape(blk_shape + (HEAD_DIM,)), lse_seq.reshape(blk_shape), delta_seq.reshape(blk_shape), jnp.arange(N_BLOCKS))
    (dk_acc, dv_acc), dq_blocks = lax.scan(one_block, (zero_kv, zero_kv), block_ins)
    grad_query = to_device_order(dq_blocks.reshape(SEQ_LEN, Q_HEADS, HEAD_DIM))
    grad_key = to_device_order((dk_acc * SCALING).astype(jnp.bfloat16))
    grad_value = to_device_order(dv_acc.astype(jnp.bfloat16))
    return grad_query, grad_key, grad_value
```

```python
import functools
import math
import jax
import jax.numpy as jnp
from jax import lax
from jax.experimental import pallas as pl
from jax.experimental.pallas import tpu as pltpu
from jax.sharding import PartitionSpec as P

TK = 256
TQ = 512
LOG2E = 1.4426950408889634


def grad_kernel(n_row, n_src, group, scaling, rows_ref, stats_ref, kv_ref, dq_ref, dkv_ref, dqt_ref):
    my_row = lax.axis_index('cy')
    tok, dim = rows_ref.shape[3], rows_ref.shape[4]
    chunk = n_src * tok
    k_src = TK // tok
    dkv_ref[...] = jnp.zeros_like(dkv_ref)
    dqt_ref[...] = jnp.zeros_like(dqt_ref)
    s_mul = jnp.float32(scaling * LOG2E)

    def tile(head, q_half, q_first, q_n, row, k_half, k_first, k_n, mask):
        ks = pl.ds(k_first, k_n)
        qs = pl.ds(q_first, q_n)
        k_t = kv_ref[row, ks, 0, k_half].reshape(k_n * tok, dim)
        v_t = kv_ref[row, ks, 1, k_half].reshape(k_n * tok, dim)
        q_t = rows_ref[qs, head, q_half].reshape(q_n * tok, dim)
        do_t = rows_ref[qs, group + head, q_half].reshape(q_n * tok, dim)
        lse = jnp.concatenate([stats_ref[q_first + i, q_half, pl.ds(head, 1), :] for i in range(q_n)], axis=1)
        delta = jnp.concatenate([stats_ref[q_first + i, q_half, pl.ds(group + head, 1), :] for i in range(q_n)], axis=1)
        nt = (((1,), (1,)), ((), ()))
        s_t = lax.dot_general(k_t, q_t, nt, preferred_element_type=jnp.float32)
        p_t = jnp.exp2(s_t * s_mul - lse)
        if mask is not None:
            p_t = jnp.where(mask, p_t, 0.0)
        dp_t = lax.dot_general(v_t, do_t, nt, preferred_element_type=jnp.float32)
        ds_t = (p_t * (dp_t - delta)).astype(jnp.bfloat16)
        p_b = p_t.astype(jnp.bfloat16)
        dv = jnp.dot(p_b, do_t, preferred_element_type=jnp.float32)
        dk = jnp.dot(ds_t, q_t, preferred_element_type=jnp.float32)
        dqt = lax.dot_general(k_t, ds_t, (((0,), (0,)), ((), ())), preferred_element_type=jnp.float32)
        dkv_ref[row, ks, 0, k_half] += dk.reshape(k_n, tok, dim)
        dkv_ref[row, ks, 1, k_half] += dv.reshape(k_n, tok, dim)
        lanes = pl.ds(pl.multiple_of(q_first * tok, q_n * tok), q_n * tok)
        dqt_ref[head, q_half, :, lanes] += dqt

    q_n = TQ // tok
    n_qt = n_src // q_n
    n_kt = n_src // k_src
    n_pairs = 2 * n_row - 1

    def full_step(idx, carry):
        kt = lax.rem(idx, n_kt)
        head = lax.rem(lax.div(idx, n_kt), group)
        pair = lax.div(idx, n_kt * group)
        other = lax.rem(my_row + 1 + lax.max(pair - n_row, 0), n_row)
        before = other < my_row
        first = pair < n_row
        row = jnp.where(first, pair, other)
        q_half = jnp.where(jnp.logical_or(first, jnp.logical_not(before)), 1, 0)
        k_half = jnp.where(jnp.logical_or(first, before), 0, 1)
        for qt in range(n_qt):
            tile(head, q_half, qt * q_n, q_n, row, k_half, kt * k_src, k_src, None)
        return carry

    lax.fori_loop(0, n_pairs * group * n_kt, full_step, 0)

    def diag_step(idx, carry):
        kt = lax.rem(idx, n_kt)
        head = lax.rem(lax.div(idx, n_kt), group)
        half = lax.div(idx, n_kt * group)
        low = jnp.where(half == 0, kt, 0)
        high = jnp.where(half == 0, n_kt, kt + 1)

        def inner(qt, c):
            q_i = lax.broadcasted_iota(jnp.int32, (TK, TK), 1)
            k_i = lax.broadcasted_iota(jnp.int32, (TK, TK), 0)
            q_pc = qt * k_src + q_i // tok
            k_pc = kt * k_src + k_i // tok
            q_pc = jnp.where(half == 0, q_pc, n_src - 1 - q_pc)
            k_pc = jnp.where(half == 0, k_pc, n_src - 1 - k_pc)
            mask = q_pc * tok + lax.rem(q_i, tok) >= k_pc * tok + lax.rem(k_i, tok)
            tile(head, half, qt * k_src, k_src, my_row, half, kt * k_src, k_src, mask)
            return c

        return lax.fori_loop(low, high, inner, carry)

    lax.fori_loop(0, 2 * group * n_kt, diag_step, 0)

    def out_step(idx, carry):
        src = lax.rem(idx, n_src)
        head = lax.rem(lax.div(idx, n_src), group)
        half = lax.div(idx, n_src * group)
        blk = dqt_ref[head, half, :, pl.ds(pl.multiple_of(src * tok, tok), tok)]
        dq_ref[src, head, half] = (jnp.transpose(blk, (1, 0)) * scaling).astype(jnp.bfloat16)
        return carry

    lax.fori_loop(0, 2 * group * n_src, out_step, 0)


def solution(mesh):
    n_row = mesh.shape['cy']
    n_cx = mesh.shape['cx']
    row_spec = P(('dp', 'cy', 'cx'), None, None)
    stat_spec = P(('dp', 'cy', 'cx'), None)

    def local_grads(query_rows, key_rows, value_rows, out_rows, grad_out, log_sum_exp):
        tok_dev, n_heads, dim = query_rows.shape
        kv_heads = key_rows.shape[1]
        group = n_heads // kv_heads
        tok = tok_dev // 2
        scaling = 1.0 / math.sqrt(dim)
        assert kv_heads == n_cx
        delta = jnp.einsum('thd,thd->th', grad_out, out_rows, preferred_element_type=jnp.float32)

        def by_head(x, per):
            return x.reshape(2, tok, kv_heads, per, dim).transpose(2, 3, 0, 1, 4)

        send = jnp.concatenate([by_head(query_rows, group), by_head(grad_out, group), by_head(key_rows, 1), by_head(value_rows, 1)], axis=1)
        stats = jnp.concatenate([(log_sum_exp * LOG2E).reshape(2, tok, kv_heads, group), delta.reshape(2, tok, kv_heads, group)], axis=3).transpose(2, 0, 3, 1)
        rows = lax.all_to_all(send, 'cx', 0, 0, tiled=True)
        stats = lax.all_to_all(stats, 'cx', 0, 0, tiled=True)
        kv = lax.all_gather(rows[:, 2 * group:], 'cy', axis=0)
        vm = pl.BlockSpec(memory_space=pltpu.VMEM)
        dq, dkv = pl.pallas_call(
            functools.partial(grad_kernel, n_row, n_cx, group, scaling),
            out_shape=(jax.ShapeDtypeStruct((n_cx, group, 2, tok, dim), jnp.bfloat16), jax.ShapeDtypeStruct((n_row, n_cx, 2, 2, tok, dim), jnp.float32)),
            in_specs=[vm] * 3,
            out_specs=(vm, vm),
            scratch_shapes=[pltpu.VMEM((group, 2, dim, n_cx * tok), jnp.float32)],
            compiler_params=pltpu.CompilerParams(vmem_limit_bytes=60 * 1024 * 1024),
            name='grad_kernel',
        )(rows, stats, kv)
        dkv = lax.psum_scatter(dkv, 'cy', scatter_dimension=0)
        dk = (dkv[:, 0] * scaling).astype(jnp.bfloat16)
        dv = dkv[:, 1].astype(jnp.bfloat16)
        back = jnp.concatenate([dq, dk[:, None], dv[:, None]], axis=1)
        back = lax.all_to_all(back, 'cx', 0, 0, tiled=True)

        def by_tok(x):
            return x.transpose(2, 3, 0, 1, 4).reshape(tok_dev, -1, dim)

        return by_tok(back[:, :group]), by_tok(back[:, group:group + 1]), by_tok(back[:, group + 1:])

    return jax.shard_map(local_grads, mesh=mesh, in_specs=(row_spec,) * 5 + (stat_spec,), out_specs=(row_spec,) * 3, check_vma=False)
```

```python
import functools
import math
import jax
import jax.numpy as jnp
from jax import lax
from jax.experimental import pallas as pl
from jax.experimental.pallas import tpu as pltpu
from jax.sharding import PartitionSpec as P

TK = 256
TQ = 512
KERNEL_VMEM = 48 * 1024 * 1024
LOG2E = 1.4426950408889634


def grad_kernel(n_row, n_src, group, scaling, own, last, src_lo, src_n, rows_ref, stats_ref, kv_ref, *refs):
    if own:
        dqt_ref, dkv_ref = refs
        dqt_ref[...] = jnp.zeros_like(dqt_ref)
    elif last:
        dqt_ref, dq_ref, dkv_ref = refs
    else:
        dqt_in, dqt_ref, dkv_ref = refs
        dqt_ref[...] = dqt_in[...]
    my_row = lax.axis_index('cy')
    tok, dim = rows_ref.shape[3], rows_ref.shape[4]
    k_src = TK // tok
    dkv_ref[...] = jnp.zeros_like(dkv_ref)
    s_mul = jnp.float32(scaling * LOG2E)

    def tile(head, q_half, q_first, q_n, k_at, o_at, k_half, k_n, mask):
        qs = pl.ds(q_first, q_n)
        k_t = kv_ref[k_at + (0, k_half)].reshape(k_n * tok, dim)
        v_t = kv_ref[k_at + (1, k_half)].reshape(k_n * tok, dim)
        q_t = rows_ref[qs, head, q_half].reshape(q_n * tok, dim)
        do_t = rows_ref[qs, group + head, q_half].reshape(q_n * tok, dim)
        lse = jnp.concatenate([stats_ref[q_first + i, q_half, pl.ds(head, 1), :] for i in range(q_n)], axis=1)
        delta = jnp.concatenate([stats_ref[q_first + i, q_half, pl.ds(group + head, 1), :] for i in range(q_n)], axis=1)
        nt = (((1,), (1,)), ((), ()))
        s_t = lax.dot_general(k_t, q_t, nt, preferred_element_type=jnp.float32)
        p_t = jnp.exp2(s_t * s_mul - lse)
        if mask is not None:
            p_t = jnp.where(mask, p_t, 0.0)
        dp_t = lax.dot_general(v_t, do_t, nt, preferred_element_type=jnp.float32)
        ds_t = (p_t * (dp_t - delta)).astype(jnp.bfloat16)
        p_b = p_t.astype(jnp.bfloat16)
        dv = jnp.dot(p_b, do_t, preferred_element_type=jnp.float32)
        dk = jnp.dot(ds_t, q_t, preferred_element_type=jnp.float32)
        dqt = lax.dot_general(k_t, ds_t, (((0,), (0,)), ((), ())), preferred_element_type=jnp.float32)
        dkv_ref[o_at + (0, k_half)] += dk.reshape(k_n, tok, dim)
        dkv_ref[o_at + (1, k_half)] += dv.reshape(k_n, tok, dim)
        lanes = pl.ds(pl.multiple_of(q_first * tok, q_n * tok), q_n * tok)
        dqt_ref[head, q_half, :, lanes] += dqt

    q_n = TQ // tok
    n_qt = n_src // q_n
    n_kt = src_n // k_src
    n_pairs = 1 if own else 2 * (n_row - 1)

    def full_step(idx, carry):
        kt = lax.rem(idx, n_kt)
        head = lax.rem(lax.div(idx, n_kt), group)
        ks = pl.ds(src_lo + kt * k_src, k_src)
        ko = pl.ds(kt * k_src, k_src)
        if own:
            q_half, k_half = 1, 0
            k_at, o_at = (ks,), (ko,)
        else:
            pair = lax.div(idx, n_kt * group)
            other = lax.rem(my_row + 1 + lax.rem(pair, n_row - 1), n_row)
            before = other < my_row
            first = pair < n_row - 1
            q_half = jnp.where(jnp.logical_or(first, jnp.logical_not(before)), 1, 0)
            k_half = jnp.where(jnp.logical_or(first, before), 0, 1)
            k_at, o_at = (other, ks), (other, ko)
        for qt in range(n_qt):
            tile(head, q_half, qt * q_n, q_n, k_at, o_at, k_half, k_src, None)
        return carry

    lax.fori_loop(0, n_pairs * group * n_kt, full_step, 0)

    def diag_step(idx, carry):
        kt = lax.rem(idx, n_kt)
        head = lax.rem(lax.div(idx, n_kt), group)
        half = lax.div(idx, n_kt * group)
        low = jnp.where(half == 0, kt, 0)
        high = jnp.where(half == 0, n_kt, kt + 1)

        def inner(qt, c):
            q_i = lax.broadcasted_iota(jnp.int32, (TK, TK), 1)
            k_i = lax.broadcasted_iota(jnp.int32, (TK, TK), 0)
            q_pc = qt * k_src + q_i // tok
            k_pc = kt * k_src + k_i // tok
            q_pc = jnp.where(half == 0, q_pc, n_src - 1 - q_pc)
            k_pc = jnp.where(half == 0, k_pc, n_src - 1 - k_pc)
            mask = q_pc * tok + lax.rem(q_i, tok) >= k_pc * tok + lax.rem(k_i, tok)
            ks = (pl.ds(kt * k_src, k_src),)
            tile(head, half, qt * k_src, k_src, ks, ks, half, k_src, mask)
            return c

        return lax.fori_loop(low, high, inner, carry)

    if own:
        lax.fori_loop(0, 2 * group * n_kt, diag_step, 0)

    def out_step(idx, carry):
        src = lax.rem(idx, n_src)
        head = lax.rem(lax.div(idx, n_src), group)
        half = lax.div(idx, n_src * group)
        blk = dqt_ref[head, half, :, pl.ds(pl.multiple_of(src * tok, tok), tok)]
        dq_ref[src, head, half] = (jnp.transpose(blk, (1, 0)) * scaling).astype(jnp.bfloat16)
        return carry

    if last:
        lax.fori_loop(0, 2 * group * n_src, out_step, 0)


def solution(mesh):
    n_row = mesh.shape['cy']
    n_cx = mesh.shape['cx']
    row_spec = P(('dp', 'cy', 'cx'), None, None)
    stat_spec = P(('dp', 'cy', 'cx'), None)
    vm = pl.BlockSpec(memory_space=pltpu.VMEM)

    def local_grads(query_rows, key_rows, value_rows, out_rows, grad_out, log_sum_exp):
        tok_dev, n_heads, dim = query_rows.shape
        kv_heads = key_rows.shape[1]
        group = n_heads // kv_heads
        tok = tok_dev // 2
        scaling = 1.0 / math.sqrt(dim)
        assert kv_heads == n_cx
        delta = jnp.einsum('thd,thd->th', grad_out, out_rows, preferred_element_type=jnp.float32)

        def by_head(x, per):
            return x.reshape(2, tok, kv_heads, per, dim).transpose(2, 3, 0, 1, 4)

        kv_own = jnp.concatenate([by_head(key_rows, 1), by_head(value_rows, 1)], axis=1)
        kv_own = lax.all_to_all(kv_own, 'cx', 0, 0, tiled=True)
        kv_all = lax.all_gather(kv_own, 'cy', axis=0)
        send = jnp.concatenate([by_head(query_rows, group), by_head(grad_out, group)], axis=1)
        stats = jnp.concatenate([(log_sum_exp * LOG2E).reshape(2, tok, kv_heads, group), delta.reshape(2, tok, kv_heads, group)], axis=3).transpose(2, 0, 3, 1)
        stats = lax.all_to_all(stats, 'cx', 0, 0, tiled=True)
        rows = lax.all_to_all(send, 'cx', 0, 0, tiled=True)

        dqt_shape = jax.ShapeDtypeStruct((group, 2, dim, n_cx * tok), jnp.float32)

        def call(kv, dqt, own, last, src_lo, src_n):
            src_shape = (src_n, 2, 2, tok, dim)
            dkv_shape = jax.ShapeDtypeStruct(src_shape if own else (n_row,) + src_shape, jnp.float32)
            dq_shape = jax.ShapeDtypeStruct((n_cx, group, 2, tok, dim), jnp.bfloat16) if last else dqt_shape
            pairs = (1 + 2 * 0.625) if own else 2 * (n_row - 1)
            flops = int(10 * pairs * group * dim * (n_cx * tok) * (src_n * tok))
            args = (rows, stats, kv) + (() if own else (dqt,))
            return pl.pallas_call(
                functools.partial(grad_kernel, n_row, n_cx, group, scaling, own, last, src_lo, src_n),
                out_shape=(dq_shape, dkv_shape),
                in_specs=[vm] * len(args),
                out_specs=(vm, vm),
                compiler_params=pltpu.CompilerParams(vmem_limit_bytes=KERNEL_VMEM),
                cost_estimate=pl.CostEstimate(flops=2 * flops, bytes_accessed=16 * 1024 * 1024, transcendentals=0),
                name='grad_own' if own else 'grad_other',
            )(*args)

        def scatter(x):
            return lax.psum_scatter(x, 'cy', scatter_dimension=0)

        half_src = n_cx // 2
        dqt, dkv_own = call(kv_own, None, True, False, 0, n_cx)
        dqt, dkv_a = call(kv_all, dqt, False, False, 0, half_src)
        dkv_a = scatter(dkv_a)
        dq, dkv_b = call(kv_all, dqt, False, True, half_src, half_src)
        dkv_b = scatter(dkv_b)
        dq = lax.all_to_all(dq, 'cx', 0, 0, tiled=True)
        dkv = jnp.concatenate([dkv_a, dkv_b], axis=0) + dkv_own
        dkv = dkv * jnp.array([scaling, 1.0], jnp.float32)[None, :, None, None, None]
        dkv = lax.all_to_all(dkv.astype(jnp.bfloat16), 'cx', 0, 0, tiled=True)

        def by_tok(x):
            return x.transpose(2, 3, 0, 1, 4).reshape(tok_dev, -1, dim)

        return by_tok(dq), by_tok(dkv[:, :1]), by_tok(dkv[:, 1:])

    return jax.shard_map(local_grads, mesh=mesh, in_specs=(row_spec,) * 5 + (stat_spec,), out_specs=(row_spec,) * 3, check_vma=False)
```
